128 devices in a mesh: dp: 8 (over x, core), tensor: 16 (over z, y).
Axes of the slice: x: 4, y: 4, z: 4, core: 2. Of those that a mesh axis runs over, the one named last changes fastest.
Arguments:
- head_outputs: bfloat16 [16384, 4096], P('dp', 'tensor'), may hold values from -6 to 6
- out_weight: bfloat16 [4096, 4096], P('tensor'), may hold values from -0.09375 to 0.09375
- residual: bfloat16 [16384, 4096], P(('dp', 'tensor')), may hold values from -6 to 6
- norm_gain: float32 [4096], replicated, may hold values from 0.25 to 1.75
- chosen: int32 [64, 256], replicated, may hold values from 0 to 16383, as said below
- gates: float32 [64, 256], replicated, may hold values from 0.25 to 1
- place: int32 [64], replicated, may hold values from 0 to 63, each once
- w_gate: bfloat16 [128, 704, 4096], P(('dp', 'tensor')), may hold values from -0.09375 to 0.09375
- w_up: bfloat16 [128, 704, 4096], P(('dp', 'tensor')), may hold values from -0.09375 to 0.09375
- w_down: bfloat16 [128, 704, 4096], P(('dp', 'tensor')), may hold values from -0.15625 to 0.15625
Outputs:
- mixed: bfloat16 [16384, 4096], P(('dp', 'tensor'))
The draws below stay inside these ranges and needn't reach their ends.
Inputs may be any that keep to these rules, and one draw needn't show every extreme that they name: `chosen`: row e lists 256 different tokens; at most 4 of them lie in one aligned block of 128 rows (the rows of one device), and in every row some block holds exactly 4.
All inputs are finite; a program needn't handle non-finite values.
Results may differ from the reference program's by a relative error of at most 0.012.
Values may be sent and summed in bfloat16 or wider, within the bound.
No kernel may reach another device: no remote copies, remote signals or barrier semaphores. Data moves between devices by JAX's collectives and lax.ppermute only.
A program may use at most 128 MiB of HBM per device.

```python
import jax
import jax.numpy as jnp
from jax import lax

D = 4096
HEADS = 32
HEAD_DIM = 128
FF = 1408
TOK_DEV = 128
OWNERS = 128
EXPERTS = 64
TOKENS = 16384
CAP = 256
MOST = 4
N_TENSOR = 16


def draw_chosen(key, part):
    keys = jax.random.split(key, 4)
    popularity = jax.random.randint(keys[0], (OWNERS,), 0, 3)
    noise = jax.random.randint(keys[1], (EXPERTS, OWNERS), 0, 64)
    device_ids = jnp.arange(OWNERS, dtype=jnp.int32)
    ranking = (noise + 32 * popularity[None, :]) * OWNERS + device_ids[None, :]
    _, order = lax.top_k(ranking, OWNERS)
    position = jnp.argsort(order, axis=1)
    quarter = OWNERS // 4
    counts = jnp.where(position < quarter, MOST, jnp.where(position < 3 * quarter, MOST // 2, 0))
    shuffle = jax.random.randint(keys[2], (EXPERTS, OWNERS, TOK_DEV), 0, 4096) * TOK_DEV + jnp.arange(TOK_DEV, dtype=jnp.int32)[None, None, :]
    picks = jnp.argsort(shuffle, axis=2)[:, :, :MOST].astype(jnp.int32)
    candidates = device_ids[None, :, None] * TOK_DEV + picks
    live = (jnp.arange(MOST, dtype=jnp.int32)[None, None, :] < counts[:, :, None]).astype(jnp.int32)
    spread = OWNERS * MOST
    order_key = jax.random.randint(keys[3], (EXPERTS, spread), 0, 4096) * spread + jnp.arange(spread, dtype=jnp.int32)[None, :]
    priority = live.reshape(EXPERTS, spread) * (4096 * spread) + order_key
    _, slots = lax.top_k(priority, CAP)
    return jnp.take_along_axis(candidates.reshape(EXPERTS, spread), slots, axis=1).astype(jnp.int32)


def levels(rng, shape, cuts, smallest, largest):
    def one(axis_at, parts):
        draws = jax.random.uniform(jax.random.fold_in(jax.random.fold_in(rng, 6), axis_at), (parts,), jnp.float32, smallest / len(cuts), largest / len(cuts))
        return jnp.repeat(jnp.exp(draws), shape[axis_at] // parts).reshape((-1,) + (1,) * (len(shape) - axis_at - 1))

    factor_of = one(*cuts[0])
    for cut in cuts[1:]:
        factor_of = factor_of * one(*cut)
    return factor_of


def bell_draw(own_key, shape, scale, bound, pieces=(), kind=jnp.bfloat16):
    array = scale * jax.random.normal(own_key, shape, jnp.float32)
    if pieces:
        array = array * levels(own_key, shape, pieces, -0.22, 0.18)
    return jnp.clip(array, -bound, bound).astype(kind)


def setup_inputs(seed: int = 0) -> dict:
    streams_of = jax.random.split(jax.random.key(seed), 11)
    return {
        "head_outputs": bell_draw(streams_of[0], (TOKENS, HEADS * HEAD_DIM), 1.0, 6.0, ((0, 8), (1, 16))),
        "out_weight": bell_draw(streams_of[1], (HEADS * HEAD_DIM, D), (HEADS * HEAD_DIM) ** -0.5, 0.09375, ((0, 16),)),
        "residual": bell_draw(streams_of[2], (TOKENS, D), 1.0, 6.0, ((0, 128),)),
        "norm_gain": jnp.clip(1.0 + 0.15 * jax.random.normal(streams_of[3], (D,), jnp.float32), 0.25, 1.75),
        "chosen": draw_chosen(jax.random.fold_in(streams_of[10], 71), 0),
        "gates": jnp.clip(jax.random.uniform(streams_of[5], (EXPERTS, CAP), jnp.float32, 0.25, 1.0), 0.25, 1.0),
        "place": jax.random.permutation(streams_of[6], EXPERTS).astype(jnp.int32),
        "w_gate": bell_draw(streams_of[7], (OWNERS, FF // 2, D), D ** -0.5, 0.09375, ((0, 128),)),
        "w_up": bell_draw(streams_of[8], (OWNERS, FF // 2, D), D ** -0.5, 0.09375, ((0, 128),)),
        "w_down": bell_draw(streams_of[9], (OWNERS, FF // 2, D), FF ** -0.5, 0.15625, ((0, 128),)),
    }


def rounded(value):
    return lax.optimization_barrier(value.astype(jnp.bfloat16)).astype(jnp.float32)

def reference(head_outputs, out_weight, residual, norm_gain, chosen, gates, place, w_gate, w_up, w_down):
    block_cols = head_outputs.shape[1] // N_TENSOR
    projected = jnp.zeros((head_outputs.shape[0], out_weight.shape[1]), jnp.float32)
    for block in range(N_TENSOR):
        left = head_outputs[:, block * block_cols:(block + 1) * block_cols]
        right = out_weight[block * block_cols:(block + 1) * block_cols]
        projected = projected + rounded(jnp.dot(left, right, preferred_element_type=jnp.float32))
    layer_state = residual.astype(jnp.float32) + projected
    scale = lax.rsqrt(lax.optimization_barrier(jnp.mean(layer_state * layer_state, axis=1, keepdims=True)) + 1.0)
    normed = (layer_state * scale * norm_gain.astype(jnp.float32)[None, :]).astype(jnp.bfloat16)
    contract = (((1,), (1,)), ((), ()))

    def expert_step(carry, inputs):
        token_rows, gate_row, slot = inputs
        inputs_rows = normed[token_rows]
        summed = jnp.zeros((token_rows.shape[0], normed.shape[1]), jnp.float32)
        for half in range(2):
            index = (2 * slot + half).astype(jnp.int32)
            gate_half = lax.dynamic_index_in_dim(w_gate, index, 0, keepdims=False)
            up_half = lax.dynamic_index_in_dim(w_up, index, 0, keepdims=False)
            down_half = lax.dynamic_index_in_dim(w_down, index, 0, keepdims=False)
            gate_part = lax.dot_general(inputs_rows, gate_half, contract, preferred_element_type=jnp.float32)
            up_part = lax.dot_general(inputs_rows, up_half, contract, preferred_element_type=jnp.float32)
            hidden = (jax.nn.silu(gate_part) * up_part).astype(jnp.bfloat16)
            half_out = jnp.dot(hidden, down_half, preferred_element_type=jnp.float32).astype(jnp.bfloat16)
            summed = summed + half_out.astype(jnp.float32)
        return (carry.at[token_rows].add(gate_row.astype(jnp.float32)[:, None] * summed), None)
    moe, _ = lax.scan(expert_step, jnp.zeros(layer_state.shape, jnp.float32), (chosen, gates, place))
    return (layer_state + moe).astype(jnp.bfloat16)
```

```python
import jax
import jax.numpy as jnp
from jax import lax
from jax.sharding import PartitionSpec as P

ROUTE = ("x", "tensor")
BF16 = jnp.bfloat16


def slots_of_block(chosen_pair, gates_pair, first_row, row_count, most):
    local_row = chosen_pair - first_row
    is_mine = (local_row >= 0) & (local_row < row_count)
    capacity_ids = jnp.arange(chosen_pair.shape[1], dtype=jnp.int32)
    earlier = (capacity_ids[:, None] < capacity_ids[None, :]).astype(BF16)
    rank = jnp.dot(is_mine.astype(BF16), earlier, preferred_element_type=jnp.float32)
    matches = is_mine[:, None, :] & (
        rank.astype(jnp.int32)[:, None, :] == jnp.arange(most, dtype=jnp.int32)[None, :, None]
    )
    row = jnp.sum(jnp.where(matches, local_row[:, None, :] + 1, 0), axis=2) - 1
    gate = jnp.sum(jnp.where(matches, gates_pair[:, None, :], 0.0), axis=2)
    return row, gate


def on_device(
    head_outputs, out_weight, residual, norm_gain, chosen, gates, place, w_gate, w_up, w_down
):
    x_count = lax.axis_size("x")
    core_count = lax.axis_size("core")
    tensor_count = lax.axis_size("tensor")
    x_at = lax.axis_index("x")
    core_at = lax.axis_index("core")
    owners = x_count * core_count * tensor_count
    row_count, model_width = residual.shape
    experts = place.shape[0]
    capacity = chosen.shape[1]
    most = 2 * capacity // owners
    swap = [(i, core_count - 1 - i) for i in range(core_count)]

    projected = lax.psum_scatter(
        jnp.dot(head_outputs, out_weight, preferred_element_type=jnp.float32).astype(BF16),
        "tensor",
        scatter_dimension=0,
        tiled=True,
    ).astype(jnp.float32)
    layer_state = residual.astype(jnp.float32) + projected
    scale = lax.rsqrt(jnp.mean(layer_state * layer_state, axis=1, keepdims=True) + 1.0)
    normed = (layer_state * scale * norm_gain[None, :]).astype(BF16)

    by_x = jnp.arange(x_count, dtype=jnp.int32) * core_count + core_at
    pairs = (by_x[:, None] * (tensor_count // 2) + jnp.arange(tensor_count // 2, dtype=jnp.int32)).reshape(-1)
    pair_map = (place[None, :] == pairs[:, None]).astype(jnp.float32)
    chosen_pair = jnp.dot(
        pair_map, chosen.astype(jnp.float32), precision=lax.Precision.HIGHEST
    ).astype(jnp.int32)
    gates_pair = jnp.dot(pair_map, gates, precision=lax.Precision.HIGHEST)
    tensor_at = lax.axis_index("tensor")
    my_first = ((x_at * core_count + core_at) * tensor_count + tensor_at) * row_count
    other_first = ((x_at * core_count + 1 - core_at) * tensor_count + tensor_at) * row_count
    my_row, my_gate = slots_of_block(chosen_pair, gates_pair, my_first, row_count, most)
    other_row, other_gate = slots_of_block(chosen_pair, gates_pair, other_first, row_count, most)
    other_row = jnp.where(other_row >= 0, other_row + row_count, -1)
    units = 2 * most
    slot_row = jnp.concatenate([my_row, other_row], axis=1)
    slot_gate = jnp.concatenate([my_gate, other_gate], axis=1)
    slot_row = jnp.broadcast_to(slot_row[:, None], (experts // 2, 2, units)).reshape(-1)
    slot_gate = jnp.broadcast_to(slot_gate[:, None], (experts // 2, 2, units)).reshape(-1)
    row_ids = jnp.arange(2 * row_count, dtype=jnp.int32)
    selector = (slot_row[:, None] == row_ids[None, :]).astype(BF16)
    combine = jnp.where(slot_row[None, :] == row_ids[:, None], slot_gate[None, :], 0.0)
    combine_high = combine.astype(BF16)
    combine_low = (combine - combine_high.astype(jnp.float32)).astype(BF16)

    both = jnp.concatenate([normed, lax.ppermute(normed, "core", swap)], axis=0)
    outgoing = jnp.dot(selector, both, preferred_element_type=jnp.float32).astype(BF16)
    received = lax.all_to_all(outgoing, ROUTE, split_axis=0, concat_axis=0, tiled=True)

    contract = (((1,), (1,)), ((), ()))
    gate_part = lax.dot_general(received, w_gate[0], contract, preferred_element_type=jnp.float32)
    up_part = lax.dot_general(received, w_up[0], contract, preferred_element_type=jnp.float32)
    hidden = (jax.nn.silu(gate_part) * up_part).astype(BF16)
    result = jnp.dot(hidden, w_down[0], preferred_element_type=jnp.float32).astype(BF16)

    returned = lax.all_to_all(result, ROUTE, split_axis=0, concat_axis=0, tiled=True)
    moe = jnp.dot(combine_high, returned, preferred_element_type=jnp.float32) + jnp.dot(
        combine_low, returned, preferred_element_type=jnp.float32
    )
    from_other = lax.ppermute(moe[row_count:].astype(BF16), "core", swap)
    return (layer_state + (moe[:row_count] + from_other.astype(jnp.float32))).astype(BF16)


def solution(mesh):
    dp, tensor = mesh.devices.shape
    split = jax.sharding.Mesh(mesh.devices.reshape(dp // 2, 2, tensor), ("x", "core", "tensor"))
    rows = P(("x", "core", "tensor"), None)
    weight = P(("x", "core", "tensor"), None, None)
    return jax.shard_map(
        on_device,
        mesh=split,
        in_specs=(
            P(("x", "core"), "tensor"),
            P("tensor", None),
            rows,
            P(),
            P(),
            P(),
            P(),
            weight,
            weight,
            weight,
        ),
        out_specs=rows,
        check_vma=False,
    )
```

```python
import jax
import jax.numpy as jnp
from jax import lax
from jax.experimental import pallas as pl
from jax.experimental.pallas import tpu as pltpu
from jax.sharding import PartitionSpec as P


ROUTE = ("x", "z", "y")
BF16 = jnp.bfloat16


def shifted(value, axis, by):
    count = lax.axis_size(axis)
    return lax.ppermute(value, axis, [(i, (i + by) % count) for i in range(count)])


def partial_kernel(side, at_ref, *refs):
    heads, mine, other, own_weight = refs[:4], refs[4:7], refs[7:10], refs[10]
    outs, sums = refs[11:15], refs[15]
    step = pl.program_id(0)
    left = jnp.concatenate([h[...].reshape(-1, h.shape[-1]) for h in heads], axis=1)
    first = step < pl.num_programs(0) // 2
    far = [jnp.where(first, a[...], b[...]) for a, b in zip(mine, other)]
    right = jnp.concatenate([own_weight[...]] + far, axis=0)
    product = jnp.dot(left, right, preferred_element_type=jnp.float32)
    sums[...] = product.astype(sums.dtype).reshape(sums.shape)
    for d, out in enumerate(outs):
        out[...] = sums[(at_ref[side] + d) % len(outs)]


def partial_sums(side, at, head_blocks, heads, mine, other, out_weight):
    n, _, rows, depth = head_blocks.shape
    half = out_weight.shape[1] // 2
    block = half // 4
    if side == 0:
        own = pl.BlockSpec((n, 1, rows, depth), lambda i, at: (0, at[1], 0, 0))
    else:
        own = pl.BlockSpec((1, n, rows, depth), lambda i, at: (at[0], 0, 0, 0))
    whole = pl.BlockSpec((n, rows, depth), lambda i, at: (0, 0, 0))

    def column(i, at):
        return jnp.where(i < 2, at[2] * 2 + i, (1 - at[2]) * 2 + i - 2)

    near = pl.BlockSpec((depth, block), lambda i, at: (0, jnp.minimum(i, 1)))
    far = pl.BlockSpec((depth, block), lambda i, at: (0, jnp.maximum(i - 2, 0)))
    mid = pl.BlockSpec((depth, block), lambda i, at: (0, side * 4 + column(i, at)))
    return pl.pallas_call(
        lambda *refs: partial_kernel(side, *refs),
        grid_spec=pltpu.PrefetchScalarGridSpec(
            num_scalar_prefetch=1,
            grid=(4,),
            in_specs=[own] + [whole] * 3 + [near] * 3 + [far] * 3 + [mid],
            out_specs=[pl.BlockSpec((rows, block), lambda i, at: (0, column(i, at)))] * n,
            scratch_shapes=[pltpu.VMEM((n, rows, block), BF16)],
        ),
        out_shape=[jax.ShapeDtypeStruct((rows, half), BF16)] * n,
        cost_estimate=pl.CostEstimate(
            flops=2 * n * rows * n * depth * half, bytes_accessed=8 * 2**20, transcendentals=0
        ),
        name="partial_sums",
    )(at, head_blocks, *heads, *mine, *other, out_weight)


def project(head_outputs, out_weight, row_count):
    n = lax.axis_size("z")
    z_at, y_at, core_at = lax.axis_index("z"), lax.axis_index("y"), lax.axis_index("core")
    at = jnp.stack([z_at, y_at, core_at]).astype(jnp.int32)
    width = out_weight.shape[1]
    part = width // 4
    head_blocks = head_outputs.reshape(n, n, row_count, head_outputs.shape[1])
    steps = (1, 3, 2)
    weights = [
        lax.dynamic_slice_in_dim(out_weight, side * (width // 2) + core_at * part, part, axis=1)
        for side in range(2)
    ]
    axes = ("y", "z")
    mine, heads = {}, {}
    for step in steps:
        for side in range(2):
            mine[side, step] = shifted(weights[side], axes[side], step)
    for step in steps:
        for side in range(2):
            target = ((y_at, z_at)[side] + step) % n
            block = lax.dynamic_index_in_dim(head_blocks, target, axis=1 - side, keepdims=False)
            heads[side, step] = shifted(block, axes[side], step)
    projected = []
    for side in range(2):
        near = [mine[side, step] for step in steps]
        far = [shifted(w, "core", 1) for w in near]
        sums = partial_sums(
            side, at, head_blocks, [heads[side, step] for step in steps], near, far, out_weight
        )
        total = sums[0].astype(jnp.float32)
        for step in steps:
            total = total + shifted(sums[step], axes[1 - side], step).astype(jnp.float32)
        projected.append(total)
    return jnp.concatenate(projected, axis=1)


def slots_of_block(chosen_pair, gates_pair, first_row, row_count, most):
    local_row = chosen_pair - first_row
    is_mine = (local_row >= 0) & (local_row < row_count)
    capacity_ids = jnp.arange(chosen_pair.shape[1], dtype=jnp.int32)
    earlier = (capacity_ids[:, None] < capacity_ids[None, :]).astype(BF16)
    rank = jnp.dot(is_mine.astype(BF16), earlier, preferred_element_type=jnp.float32)
    matches = is_mine[:, None, :] & (
        rank.astype(jnp.int32)[:, None, :] == jnp.arange(most, dtype=jnp.int32)[None, :, None]
    )
    row = jnp.sum(jnp.where(matches, local_row[:, None, :] + 1, 0), axis=2) - 1
    gate = jnp.sum(jnp.where(matches, gates_pair[:, None, :], 0.0), axis=2)
    return row, gate


def on_device(
    head_outputs, out_weight, residual, norm_gain, chosen, gates, place, w_gate, w_up, w_down
):
    x_count = lax.axis_size("x")
    core_count = lax.axis_size("core")
    tensor_count = lax.axis_size("z") * lax.axis_size("y")
    x_at = lax.axis_index("x")
    core_at = lax.axis_index("core")
    owners = x_count * core_count * tensor_count
    row_count, model_width = residual.shape
    experts = place.shape[0]
    capacity = chosen.shape[1]
    most = 2 * capacity // owners
    swap = [(i, core_count - 1 - i) for i in range(core_count)]

    projected = project(head_outputs, out_weight, row_count)
    layer_state = residual.astype(jnp.float32) + projected
    scale = lax.rsqrt(jnp.mean(layer_state * layer_state, axis=1, keepdims=True) + 1.0)
    normed = (layer_state * scale * norm_gain[None, :]).astype(BF16)

    by_x = jnp.arange(x_count, dtype=jnp.int32) * core_count + core_at
    pairs = (by_x[:, None] * (tensor_count // 2) + jnp.arange(tensor_count // 2, dtype=jnp.int32)).reshape(-1)
    pair_map = (place[None, :] == pairs[:, None]).astype(jnp.float32)
    chosen_pair = jnp.dot(
        pair_map, chosen.astype(jnp.float32), precision=lax.Precision.HIGHEST
    ).astype(jnp.int32)
    gates_pair = jnp.dot(pair_map, gates, precision=lax.Precision.HIGHEST)
    tensor_at = lax.axis_index("z") * lax.axis_size("y") + lax.axis_index("y")
    my_first = ((x_at * core_count + core_at) * tensor_count + tensor_at) * row_count
    other_first = ((x_at * core_count + 1 - core_at) * tensor_count + tensor_at) * row_count
    my_row, my_gate = slots_of_block(chosen_pair, gates_pair, my_first, row_count, most)
    other_row, other_gate = slots_of_block(chosen_pair, gates_pair, other_first, row_count, most)
    other_row = jnp.where(other_row >= 0, other_row + row_count, -1)
    units = 2 * most
    slot_row = jnp.concatenate([my_row, other_row], axis=1)
    slot_gate = jnp.concatenate([my_gate, other_gate], axis=1)
    slot_row = jnp.broadcast_to(slot_row[:, None], (experts // 2, 2, units)).reshape(-1)
    slot_gate = jnp.broadcast_to(slot_gate[:, None], (experts // 2, 2, units)).reshape(-1)
    row_ids = jnp.arange(2 * row_count, dtype=jnp.int32)
    selector = (slot_row[:, None] == row_ids[None, :]).astype(BF16)
    combine = jnp.where(slot_row[None, :] == row_ids[:, None], slot_gate[None, :], 0.0)
    combine_high = combine.astype(BF16)
    combine_low = (combine - combine_high.astype(jnp.float32)).astype(BF16)

    both = jnp.concatenate([normed, lax.ppermute(normed, "core", swap)], axis=0)
    outgoing = jnp.dot(selector, both, preferred_element_type=jnp.float32).astype(BF16)
    received = lax.all_to_all(outgoing, ROUTE, split_axis=0, concat_axis=0, tiled=True)

    contract = (((1,), (1,)), ((), ()))
    gate_part = lax.dot_general(received, w_gate[0], contract, preferred_element_type=jnp.float32)
    up_part = lax.dot_general(received, w_up[0], contract, preferred_element_type=jnp.float32)
    hidden = (jax.nn.silu(gate_part) * up_part).astype(BF16)
    result = jnp.dot(hidden, w_down[0], preferred_element_type=jnp.float32).astype(BF16)

    returned = lax.all_to_all(result, ROUTE, split_axis=0, concat_axis=0, tiled=True)
    moe = jnp.dot(combine_high, returned, preferred_element_type=jnp.float32) + jnp.dot(
        combine_low, returned, preferred_element_type=jnp.float32
    )
    from_other = lax.ppermute(moe[row_count:].astype(BF16), "core", swap)
    return (layer_state + (moe[:row_count] + from_other.astype(jnp.float32))).astype(BF16)


def solution(mesh):
    dp, tensor = mesh.devices.shape
    side = round(tensor**0.5)
    split = jax.sharding.Mesh(mesh.devices.reshape(dp // 2, 2, side, side), ("x", "core", "z", "y"))
    rows = P(("x", "core", "z", "y"), None)
    weight = P(("x", "core", "z", "y"), None, None)
    return jax.shard_map(
        on_device,
        mesh=split,
        in_specs=(
            P(("x", "core"), ("z", "y")),
            P(("z", "y"), None),
            rows,
            P(),
            P(),
            P(),
            P(),
            weight,
            weight,
            weight,
        ),
        out_specs=rows,
        check_vma=False,
    )
```

```python
import jax
import jax.numpy as jnp
from jax import lax
from jax.experimental import pallas as pl
from jax.experimental.pallas import tpu as pltpu
from jax.sharding import PartitionSpec as P


ROUTE = ("x", "z", "y")
BF16 = jnp.bfloat16


def shifted(value, axis, by):
    count = lax.axis_size(axis)
    return lax.ppermute(value, axis, [(i, (i + by) % count) for i in range(count)])


def partial_kernel(side, at_ref, own_heads, own_weight, *refs):
    heads, mine, other, outs, sums = refs[:3], refs[3:6], refs[6:9], refs[9:-1], refs[-1]
    depth = own_heads.shape[-1]
    first = pl.program_id(0) < pl.num_programs(0) // 2
    left = [own_heads[...].reshape(-1, depth)]
    left += [jnp.concatenate([h[:, :depth], h[:, depth:]], axis=0) for h in heads]
    right = [own_weight[...]] + [jnp.where(first, a[...], b[...]) for a, b in zip(mine, other)]
    product = jnp.dot(
        jnp.concatenate(left, axis=1),
        jnp.concatenate(right, axis=0),
        preferred_element_type=jnp.float32,
    )
    sums[...] = product.astype(sums.dtype).reshape(sums.shape)
    for d, out in enumerate(outs):
        out[...] = sums[(at_ref[side] + d) % len(outs)]


def partial_sums(side, at, head_blocks, out_weight, mine, other):
    n, _, rows, depth = head_blocks.shape
    half = out_weight.shape[1] // 2
    block = half // 4
    if side == 0:
        own = pl.BlockSpec((n, 1, rows, depth), lambda i, at: (0, at[1], 0, 0))
    else:
        own = pl.BlockSpec((1, n, rows, depth), lambda i, at: (at[0], 0, 0, 0))

    def column(i, at):
        return jnp.where(i < 2, at[2] * 2 + i, (1 - at[2]) * 2 + i - 2)

    heads = pl.BlockSpec((depth, block), lambda i, at: (0, 2))
    near = pl.BlockSpec((depth, block), lambda i, at: (0, jnp.minimum(i, 1)))
    far = pl.BlockSpec((depth, block), lambda i, at: (0, jnp.maximum(i - 2, 0)))
    mid = pl.BlockSpec((depth, block), lambda i, at: (0, side * 4 + column(i, at)))
    return pl.pallas_call(
        lambda *refs: partial_kernel(side, *refs),
        grid_spec=pltpu.PrefetchScalarGridSpec(
            num_scalar_prefetch=1,
            grid=(4,),
            in_specs=[own, mid] + [heads] * 3 + [near] * 3 + [far] * 3,
            out_specs=[pl.BlockSpec((rows, block), lambda i, at: (0, column(i, at)))] * n,
            scratch_shapes=[pltpu.VMEM((n, rows, block), BF16)],
        ),
        out_shape=[jax.ShapeDtypeStruct((rows, half), BF16)] * n,
        compiler_params=pltpu.CompilerParams(vmem_limit_bytes=16 * 2**20),
        cost_estimate=pl.CostEstimate(
            flops=2 * n * rows * n * depth * half, bytes_accessed=8 * 2**20, transcendentals=0
        ),
        name="partial_sums",
    )(at, head_blocks, out_weight, *mine, *mine, *other)


def project(head_outputs, out_weight, row_count):
    n = lax.axis_size("z")
    z_at, y_at, core_at = lax.axis_index("z"), lax.axis_index("y"), lax.axis_index("core")
    at = jnp.stack([z_at, y_at, core_at]).astype(jnp.int32)
    depth, width = out_weight.shape
    part = width // 4
    head_blocks = head_outputs.reshape(n, n, row_count, depth)
    steps = (1, 3, 2)
    axes = ("y", "z")
    mine = {}
    for step in steps:
        for side in range(2):
            weight = lax.dynamic_slice_in_dim(
                out_weight, side * (width // 2) + core_at * part, part, axis=1
            )
            target = ((y_at, z_at)[side] + step) % n
            heads = lax.dynamic_index_in_dim(head_blocks, target, axis=1 - side, keepdims=False)
            heads = heads.reshape(2, n * row_count // 2, depth)
            packed = jnp.concatenate([weight, heads[0], heads[1]], axis=1)
            mine[side, step] = shifted(packed, axes[side], step)
    projected = []
    for side in range(2):
        near = [mine[side, step] for step in steps]
        far = [shifted(w, "core", 1) for w in near]
        sums = partial_sums(side, at, head_blocks, out_weight, near, far)
        total = sums[0].astype(jnp.float32)
        for d in steps:
            total = total + shifted(sums[d], axes[1 - side], d).astype(jnp.float32)
        projected.append(total)
    return jnp.concatenate(projected, axis=1)


def combine_kernel(weights, returned, mine, other):
    rows = mine.shape[0]
    parts = jnp.dot(weights[...], returned[...], preferred_element_type=jnp.float32)
    sums = parts[: 2 * rows] + parts[2 * rows :]
    mine[...] = sums[:rows]
    other[...] = sums[rows:].astype(other.dtype)


def combined(weights, returned, rows):
    slots, width = returned.shape
    block = width // 8
    return pl.pallas_call(
        combine_kernel,
        grid=(width // block,),
        in_specs=[
            pl.BlockSpec((4 * rows, slots), lambda i: (0, 0)),
            pl.BlockSpec((slots, block), lambda i: (0, i)),
        ],
        out_specs=[pl.BlockSpec((rows, block), lambda i: (0, i))] * 2,
        out_shape=[
            jax.ShapeDtypeStruct((rows, width), jnp.float32),
            jax.ShapeDtypeStruct((rows, width), BF16),
        ],
        compiler_params=pltpu.CompilerParams(vmem_limit_bytes=16 * 2**20),
        cost_estimate=pl.CostEstimate(
            flops=8 * rows * slots * width, bytes_accessed=8 * 2**20, transcendentals=0
        ),
        name="combined",
    )(weights, returned)


def slots_of_block(chosen_pair, gates_pair, first_row, row_count, most):
    local_row = chosen_pair - first_row
    is_mine = (local_row >= 0) & (local_row < row_count)
    capacity_ids = jnp.arange(chosen_pair.shape[1], dtype=jnp.int32)
    earlier = (capacity_ids[:, None] < capacity_ids[None, :]).astype(BF16)
    rank = jnp.dot(is_mine.astype(BF16), earlier, preferred_element_type=jnp.float32)
    matches = is_mine[:, None, :] & (
        rank.astype(jnp.int32)[:, None, :] == jnp.arange(most, dtype=jnp.int32)[None, :, None]
    )
    row = jnp.sum(jnp.where(matches, local_row[:, None, :] + 1, 0), axis=2) - 1
    gate = jnp.sum(jnp.where(matches, gates_pair[:, None, :], 0.0), axis=2)
    return row, gate


def on_device(
    head_outputs, out_weight, residual, norm_gain, chosen, gates, place, w_gate, w_up, w_down
):
    x_count = lax.axis_size("x")
    core_count = lax.axis_size("core")
    tensor_count = lax.axis_size("z") * lax.axis_size("y")
    x_at = lax.axis_index("x")
    core_at = lax.axis_index("core")
    owners = x_count * core_count * tensor_count
    row_count, model_width = residual.shape
    experts = place.shape[0]
    capacity = chosen.shape[1]
    most = 2 * capacity // owners
    swap = [(i, core_count - 1 - i) for i in range(core_count)]

    projected = project(head_outputs, out_weight, row_count)
    layer_state = residual.astype(jnp.float32) + projected
    scale = lax.rsqrt(jnp.mean(layer_state * layer_state, axis=1, keepdims=True) + 1.0)
    normed = (layer_state * scale * norm_gain[None, :]).astype(BF16)

    by_x = jnp.arange(x_count, dtype=jnp.int32) * core_count + core_at
    pairs = (by_x[:, None] * (tensor_count // 2) + jnp.arange(tensor_count // 2, dtype=jnp.int32)).reshape(-1)
    pair_map = (place[None, :] == pairs[:, None]).astype(jnp.float32)
    chosen_pair = jnp.dot(
        pair_map, chosen.astype(jnp.float32), precision=lax.Precision.HIGHEST
    ).astype(jnp.int32)
    gates_pair = jnp.dot(pair_map, gates, precision=lax.Precision.HIGHEST)
    tensor_at = lax.axis_index("z") * lax.axis_size("y") + lax.axis_index("y")
    my_first = ((x_at * core_count + core_at) * tensor_count + tensor_at) * row_count
    other_first = ((x_at * core_count + 1 - core_at) * tensor_count + tensor_at) * row_count
    my_row, my_gate = slots_of_block(chosen_pair, gates_pair, my_first, row_count, most)
    other_row, other_gate = slots_of_block(chosen_pair, gates_pair, other_first, row_count, most)
    other_row = jnp.where(other_row >= 0, other_row + row_count, -1)
    units = 2 * most
    slot_row = jnp.concatenate([my_row, other_row], axis=1)
    slot_gate = jnp.concatenate([my_gate, other_gate], axis=1)
    slot_row = jnp.broadcast_to(slot_row[:, None], (experts // 2, 2, units)).reshape(-1)
    slot_gate = jnp.broadcast_to(slot_gate[:, None], (experts // 2, 2, units)).reshape(-1)
    row_ids = jnp.arange(2 * row_count, dtype=jnp.int32)
    selector = (slot_row[:, None] == row_ids[None, :]).astype(BF16)
    combine = jnp.where(slot_row[None, :] == row_ids[:, None], slot_gate[None, :], 0.0)
    combine_high = combine.astype(BF16)
    combine_low = (combine - combine_high.astype(jnp.float32)).astype(BF16)
    combine = jnp.concatenate([combine_high, combine_low], axis=0)

    both = jnp.concatenate([normed, lax.ppermute(normed, "core", swap)], axis=0)
    outgoing = jnp.dot(selector, both, preferred_element_type=jnp.float32).astype(BF16)
    received = lax.all_to_all(outgoing, ROUTE, split_axis=0, concat_axis=0, tiled=True)

    contract = (((1,), (1,)), ((), ()))
    gate_part = lax.dot_general(received, w_gate[0], contract, preferred_element_type=jnp.float32)
    up_part = lax.dot_general(received, w_up[0], contract, preferred_element_type=jnp.float32)
    hidden = lax.optimization_barrier((jax.nn.silu(gate_part) * up_part).astype(BF16))
    result = jnp.dot(hidden, w_down[0], preferred_element_type=jnp.float32).astype(BF16)

    returned = lax.all_to_all(result, ROUTE, split_axis=0, concat_axis=0, tiled=True)
    moe, for_other = combined(combine, returned, row_count)
    from_other = lax.ppermute(for_other, "core", swap)
    return (layer_state + (moe + from_other.astype(jnp.float32))).astype(BF16)


def solution(mesh):
    dp, tensor = mesh.devices.shape
    side = round(tensor**0.5)
    split = jax.sharding.Mesh(mesh.devices.reshape(dp // 2, 2, side, side), ("x", "core", "z", "y"))
    rows = P(("x", "core", "z", "y"), None)
    weight = P(("x", "core", "z", "y"), None, None)
    return jax.shard_map(
        on_device,
        mesh=split,
        in_specs=(
            P(("x", "core"), ("z", "y")),
            P(("z", "y"), None),
            rows,
            P(),
            P(),
            P(),
            P(),
            weight,
            weight,
            weight,
        ),
        out_specs=rows,
        check_vma=False,
    )
```

```python
import jax
import jax.numpy as jnp
from jax import lax
from jax.experimental import pallas as pl
from jax.experimental.pallas import tpu as pltpu
from jax.sharding import PartitionSpec as P


ROUTE = ("x", "z", "y")
BF16 = jnp.bfloat16


def shifted(value, axis, by):
    count = lax.axis_size(axis)
    return lax.ppermute(value, axis, [(i, (i + by) % count) for i in range(count)])


def partial_kernel(side, at_ref, own_heads, out_weight, *refs):
    mine, other, outs = refs[:3], refs[3:6], refs[6:10]
    own_at, near_at, far_at, mine_at, other_at, left, sems = refs[10:]
    n, rows, depth = own_at.shape
    half = out_weight.shape[1] // 2
    part = half // 2
    core = at_ref[2]
    near_column = pl.multiple_of(core * part, part)
    far_column = pl.multiple_of((1 - core) * part, part)
    if side == 0:
        heads_of_mine = own_heads.at[:, at_ref[1]]
    else:
        heads_of_mine = own_heads.at[at_ref[0]]
    copies = [
        pltpu.make_async_copy(heads_of_mine, own_at, sems.at[0]),
        pltpu.make_async_copy(
            out_weight.at[:, pl.ds(side * half + near_column, part)], near_at, sems.at[1]
        ),
    ]
    copies += [pltpu.make_async_copy(a, mine_at.at[k], sems.at[2 + k]) for k, a in enumerate(mine)]
    copies += [
        pltpu.make_async_copy(
            out_weight.at[:, pl.ds(side * half + far_column, part)], far_at, sems.at[5]
        )
    ]
    copies += [
        pltpu.make_async_copy(b.at[:, pl.ds(0, part)], other_at.at[k], sems.at[6 + k])
        for k, b in enumerate(other)
    ]
    for copy in copies:
        copy.start()
    for copy in copies[:5]:
        copy.wait()
    for d in range(n):
        block = (at_ref[side] + d) % n
        here = pl.ds(d * rows, rows)
        left[here, pl.ds(0, depth)] = own_at[block]
        for k in range(n - 1):
            left[here, pl.ds((k + 1) * depth, depth)] = mine_at[
                k,
                pl.ds(pl.multiple_of(block % 2 * rows, rows), rows),
                pl.ds(pl.multiple_of(part + block // 2 * depth, depth), depth),
            ]

    def product(own_weight, pieces, first_column, width):
        for low in range(0, part, width):
            window = pl.ds(low, width)
            right = jnp.concatenate(
                [own_weight[:, window]] + [pieces[k, :, window] for k in range(n - 1)], axis=0
            )
            sums = jnp.dot(left[...], right, preferred_element_type=jnp.float32).astype(BF16)
            column = pl.ds(pl.multiple_of(first_column + low, width), width)
            for d, out in enumerate(outs):
                out[:, column] = sums[d * rows : (d + 1) * rows]

    product(near_at, mine_at, near_column, part // 2)
    for copy in copies[5:]:
        copy.wait()
    product(far_at, other_at, far_column, part // 2)


def partial_sums(side, at, head_blocks, out_weight, mine, other):
    n, _, rows, depth = head_blocks.shape
    half = out_weight.shape[1] // 2
    part = half // 2
    anywhere = pl.BlockSpec(memory_space=pl.ANY)
    return pl.pallas_call(
        lambda *refs: partial_kernel(side, *refs),
        in_specs=[pl.BlockSpec(memory_space=pltpu.SMEM)] + [anywhere] * 8,
        out_specs=[pl.BlockSpec(memory_space=pltpu.VMEM)] * n,
        out_shape=[jax.ShapeDtypeStruct((rows, half), BF16)] * n,
        scratch_shapes=[
            pltpu.VMEM((n, rows, depth), BF16),
            pltpu.VMEM((depth, part), BF16),
            pltpu.VMEM((depth, part), BF16),
            pltpu.VMEM((n - 1,) + mine[0].shape, BF16),
            pltpu.VMEM((n - 1, depth, part), BF16),
            pltpu.VMEM((n * rows, n * depth), BF16),
            pltpu.SemaphoreType.DMA((9,)),
        ],
        compiler_params=pltpu.CompilerParams(vmem_limit_bytes=20 * 2**20),
        cost_estimate=pl.CostEstimate(
            flops=2 * n * rows * n * depth * half, bytes_accessed=8 * 2**20, transcendentals=0
        ),
        name="partial_sums",
    )(at, head_blocks, out_weight, *mine, *other)


def project(head_outputs, out_weight, row_count):
    n = lax.axis_size("z")
    z_at, y_at, core_at = lax.axis_index("z"), lax.axis_index("y"), lax.axis_index("core")
    at = jnp.stack([z_at, y_at, core_at]).astype(jnp.int32)
    depth, width = out_weight.shape
    part = width // 4
    head_blocks = head_outputs.reshape(n, n, row_count, depth)
    steps = (1, 3, 2)
    axes = ("y", "z")
    mine = {}
    for step in steps:
        for side in range(2):
            weight = lax.dynamic_slice_in_dim(
                out_weight, side * (width // 2) + core_at * part, part, axis=1
            )
            target = ((y_at, z_at)[side] + step) % n
            heads = lax.dynamic_index_in_dim(head_blocks, target, axis=1 - side, keepdims=False)
            heads = heads.reshape(2, n * row_count // 2, depth)
            packed = jnp.concatenate([weight, heads[0], heads[1]], axis=1)
            mine[side, step] = shifted(packed, axes[side], step)
    sums = []
    for side in range(2):
        near = [mine[side, step] for step in steps]
        if side == 1:
            near[2], sums[0] = lax.optimization_barrier((near[2], sums[0]))
        far = [shifted(w, "core", 1) for w in near]
        sums.append(partial_sums(side, at, head_blocks, out_weight, near, far))
    projected = []
    for side in range(2):
        total = sums[side][0].astype(jnp.float32)
        for d in steps:
            total = total + shifted(sums[side][d], axes[1 - side], d).astype(jnp.float32)
        projected.append(total)
    return jnp.concatenate(projected, axis=1)


def combine_kernel(weights, returned, mine, other, held, sems):
    rows = mine.shape[0]
    parts, _, width = held.shape
    copies = [
        pltpu.make_async_copy(
            returned.at[:, pl.ds(k * width, width)], held.at[k], sems.at[k]
        )
        for k in range(parts)
    ]
    for copy in copies:
        copy.start()
    for k, copy in enumerate(copies):
        copy.wait()
        products = jnp.dot(weights[...], held[k], preferred_element_type=jnp.float32)
        sums = products[: 2 * rows] + products[2 * rows :]
        mine[:, pl.ds(k * width, width)] = sums[:rows]
        other[:, pl.ds(k * width, width)] = sums[rows:].astype(other.dtype)


def combined(weights, returned, rows):
    slots, width = returned.shape
    parts = 8
    whole = pl.BlockSpec(memory_space=pltpu.VMEM)
    return pl.pallas_call(
        combine_kernel,
        in_specs=[whole, pl.BlockSpec(memory_space=pl.ANY)],
        out_specs=[whole] * 2,
        out_shape=[
            jax.ShapeDtypeStruct((rows, width), jnp.float32),
            jax.ShapeDtypeStruct((rows, width), BF16),
        ],
        scratch_shapes=[
            pltpu.VMEM((parts, slots, width // parts), BF16),
            pltpu.SemaphoreType.DMA((parts,)),
        ],
        compiler_params=pltpu.CompilerParams(vmem_limit_bytes=16 * 2**20),
        cost_estimate=pl.CostEstimate(
            flops=8 * rows * slots * width, bytes_accessed=8 * 2**20, transcendentals=0
        ),
        name="combined",
    )(weights, returned)


def slots_of_block(chosen_pair, gates_pair, first_row, row_count, most):
    local_row = chosen_pair - first_row
    is_mine = (local_row >= 0) & (local_row < row_count)
    capacity_ids = jnp.arange(chosen_pair.shape[1], dtype=jnp.int32)
    earlier = (capacity_ids[:, None] < capacity_ids[None, :]).astype(BF16)
    rank = jnp.dot(is_mine.astype(BF16), earlier, preferred_element_type=jnp.float32)
    matches = is_mine[:, None, :] & (
        rank.astype(jnp.int32)[:, None, :] == jnp.arange(most, dtype=jnp.int32)[None, :, None]
    )
    row = jnp.sum(jnp.where(matches, local_row[:, None, :] + 1, 0), axis=2) - 1
    gate = jnp.sum(jnp.where(matches, gates_pair[:, None, :], 0.0), axis=2)
    return row, gate


def on_device(
    head_outputs, out_weight, residual, norm_gain, chosen, gates, place, w_gate, w_up, w_down
):
    x_count = lax.axis_size("x")
    core_count = lax.axis_size("core")
    tensor_count = lax.axis_size("z") * lax.axis_size("y")
    x_at = lax.axis_index("x")
    core_at = lax.axis_index("core")
    owners = x_count * core_count * tensor_count
    row_count, model_width = residual.shape
    experts = place.shape[0]
    capacity = chosen.shape[1]
    most = 2 * capacity // owners
    swap = [(i, core_count - 1 - i) for i in range(core_count)]

    projected = project(head_outputs, out_weight, row_count)
    layer_state = residual.astype(jnp.float32) + projected
    scale = lax.rsqrt(jnp.mean(layer_state * layer_state, axis=1, keepdims=True) + 1.0)
    normed = (layer_state * scale * norm_gain[None, :]).astype(BF16)

    by_x = jnp.arange(x_count, dtype=jnp.int32) * core_count + core_at
    pairs = (by_x[:, None] * (tensor_count // 2) + jnp.arange(tensor_count // 2, dtype=jnp.int32)).reshape(-1)
    pair_map = (place[None, :] == pairs[:, None]).astype(jnp.float32)
    chosen_pair = jnp.dot(
        pair_map, chosen.astype(jnp.float32), precision=lax.Precision.HIGHEST
    ).astype(jnp.int32)
    gates_pair = jnp.dot(pair_map, gates, precision=lax.Precision.HIGHEST)
    tensor_at = lax.axis_index("z") * lax.axis_size("y") + lax.axis_index("y")
    my_first = ((x_at * core_count + core_at) * tensor_count + tensor_at) * row_count
    other_first = ((x_at * core_count + 1 - core_at) * tensor_count + tensor_at) * row_count
    my_row, my_gate = slots_of_block(chosen_pair, gates_pair, my_first, row_count, most)
    other_row, other_gate = slots_of_block(chosen_pair, gates_pair, other_first, row_count, most)
    other_row = jnp.where(other_row >= 0, other_row + row_count, -1)
    units = 2 * most
    slot_row = jnp.concatenate([my_row, other_row], axis=1)
    slot_gate = jnp.concatenate([my_gate, other_gate], axis=1)
    slot_row = jnp.broadcast_to(slot_row[:, None], (experts // 2, 2, units)).reshape(-1)
    slot_gate = jnp.broadcast_to(slot_gate[:, None], (experts // 2, 2, units)).reshape(-1)
    row_ids = jnp.arange(2 * row_count, dtype=jnp.int32)
    selector = (slot_row[:, None] == row_ids[None, :]).astype(BF16)
    combine = jnp.where(slot_row[None, :] == row_ids[:, None], slot_gate[None, :], 0.0)
    combine_high = combine.astype(BF16)
    combine_low = (combine - combine_high.astype(jnp.float32)).astype(BF16)
    combine = jnp.concatenate([combine_high, combine_low], axis=0)

    both = jnp.concatenate([normed, lax.ppermute(normed, "core", swap)], axis=0)
    outgoing = jnp.dot(selector, both, preferred_element_type=jnp.float32).astype(BF16)
    received = lax.all_to_all(outgoing, ROUTE, split_axis=0, concat_axis=0, tiled=True)

    contract = (((1,), (1,)), ((), ()))
    gate_part = lax.dot_general(received, w_gate[0], contract, preferred_element_type=jnp.float32)
    up_part = lax.dot_general(received, w_up[0], contract, preferred_element_type=jnp.float32)
    hidden = lax.optimization_barrier((jax.nn.silu(gate_part) * up_part).astype(BF16))
    result = jnp.dot(hidden, w_down[0], preferred_element_type=jnp.float32).astype(BF16)

    returned = lax.all_to_all(result, ROUTE, split_axis=0, concat_axis=0, tiled=True)
    moe, for_other = combined(combine, returned, row_count)
    from_other = lax.ppermute(for_other, "core", swap)
    return (layer_state + (moe + from_other.astype(jnp.float32))).astype(BF16)


def solution(mesh):
    dp, tensor = mesh.devices.shape
    side = round(tensor**0.5)
    split = jax.sharding.Mesh(mesh.devices.reshape(dp // 2, 2, side, side), ("x", "core", "z", "y"))
    rows = P(("x", "core", "z", "y"), None)
    weight = P(("x", "core", "z", "y"), None, None)
    return jax.shard_map(
        on_device,
        mesh=split,
        in_specs=(
            P(("x", "core"), ("z", "y")),
            P(("z", "y"), None),
            rows,
            P(),
            P(),
            P(),
            P(),
            weight,
            weight,
            weight,
        ),
        out_specs=rows,
        check_vma=False,
    )
```

```python
import jax
import jax.numpy as jnp
from jax import lax
from jax.experimental import pallas as pl
from jax.experimental.pallas import tpu as pltpu
from jax.sharding import PartitionSpec as P


ROUTE = ("x", "z", "y")
BF16 = jnp.bfloat16


def shifted(value, axis, by):
    count = lax.axis_size(axis)
    return lax.ppermute(value, axis, [(i, (i + by) % count) for i in range(count)])


def partial_kernel(side, at_ref, own_heads, out_weight, *refs):
    mine, other, outs, left = refs[:3], refs[3:6], refs[6:10], refs[10]
    n, _, rows, depth = own_heads.shape
    half = out_weight.shape[1] // 2
    part = half // 2
    width = part // 2
    core = at_ref[2]
    for d in range(n):
        block = (at_ref[side] + d) % n
        here = pl.ds(d * rows, rows)
        if side == 0:
            left[here, pl.ds(0, depth)] = own_heads[block, at_ref[1]]
        else:
            left[here, pl.ds(0, depth)] = own_heads[at_ref[0], block]
        for k, piece in enumerate(mine):
            left[here, pl.ds((k + 1) * depth, depth)] = piece[
                pl.ds(pl.multiple_of(block % 2 * rows, rows), rows),
                pl.ds(pl.multiple_of(part + block // 2 * depth, depth), depth),
            ]
    for owner, pieces in ((core, mine), (1 - core, other)):
        for low in range(0, part, width):
            first_column = owner * part + low
            own = out_weight[:, pl.ds(pl.multiple_of(side * half + first_column, width), width)]
            right = jnp.concatenate([own] + [p[:, pl.ds(low, width)] for p in pieces], axis=0)
            sums = jnp.dot(left[...], right, preferred_element_type=jnp.float32).astype(BF16)
            column = pl.ds(pl.multiple_of(first_column, width), width)
            for d, out in enumerate(outs):
                out[:, column] = sums[d * rows : (d + 1) * rows]


def partial_sums(side, at, head_blocks, out_weight, mine, other):
    n, _, rows, depth = head_blocks.shape
    half = out_weight.shape[1] // 2
    whole = pl.BlockSpec(memory_space=pltpu.VMEM)
    return pl.pallas_call(
        lambda *refs: partial_kernel(side, *refs),
        in_specs=[pl.BlockSpec(memory_space=pltpu.SMEM)] + [whole] * 8,
        out_specs=[whole] * n,
        out_shape=[jax.ShapeDtypeStruct((rows, half), BF16)] * n,
        scratch_shapes=[pltpu.VMEM((n * rows, n * depth), BF16)],
        compiler_params=pltpu.CompilerParams(vmem_limit_bytes=16 * 2**20),
        cost_estimate=pl.CostEstimate(
            flops=2 * n * rows * n * depth * half, bytes_accessed=8 * 2**20, transcendentals=0
        ),
        name="partial_sums",
    )(at, head_blocks, out_weight, *mine, *other)


def project(head_outputs, out_weight, row_count):
    n = lax.axis_size("z")
    z_at, y_at, core_at = lax.axis_index("z"), lax.axis_index("y"), lax.axis_index("core")
    at = jnp.stack([z_at, y_at, core_at]).astype(jnp.int32)
    depth, width = out_weight.shape
    part = width // 4
    head_blocks = head_outputs.reshape(n, n, row_count, depth)
    steps = (1, 3, 2)
    axes = ("y", "z")
    mine = {}
    for step in steps:
        for side in range(2):
            weight = lax.dynamic_slice_in_dim(
                out_weight, side * (width // 2) + core_at * part, part, axis=1
            )
            target = ((y_at, z_at)[side] + step) % n
            heads = lax.dynamic_index_in_dim(head_blocks, target, axis=1 - side, keepdims=False)
            heads = heads.reshape(2, n * row_count // 2, depth)
            packed = jnp.concatenate([weight, heads[0], heads[1]], axis=1)
            mine[side, step] = shifted(packed, axes[side], step)
    projected = []
    for side in range(2):
        near = [mine[side, step] for step in steps]
        far = []
        for step, piece in zip(steps, near):
            far.append(shifted(piece, "core", 1))
        sums = partial_sums(side, at, head_blocks, out_weight, near, far)
        total = sums[0].astype(jnp.float32)
        for d in steps:
            sent = shifted(sums[d], axes[1 - side], d)
            total = total + sent.astype(jnp.float32)
        projected.append(total)
    return jnp.concatenate(projected, axis=1)


def combine_kernel(weights, returned, mine, other, held, sems):
    rows = mine.shape[0]
    parts, _, width = held.shape
    copies = [
        pltpu.make_async_copy(
            returned.at[:, pl.ds(k * width, width)], held.at[k], sems.at[k]
        )
        for k in range(parts)
    ]
    for copy in copies:
        copy.start()
    for k, copy in enumerate(copies):
        copy.wait()
        products = jnp.dot(weights[...], held[k], preferred_element_type=jnp.float32)
        sums = products[: 2 * rows] + products[2 * rows :]
        mine[:, pl.ds(k * width, width)] = sums[:rows]
        other[:, pl.ds(k * width, width)] = sums[rows:].astype(other.dtype)


def combined(weights, returned, rows):
    slots, width = returned.shape
    parts = 8
    whole = pl.BlockSpec(memory_space=pltpu.VMEM)
    return pl.pallas_call(
        combine_kernel,
        in_specs=[whole, pl.BlockSpec(memory_space=pl.ANY)],
        out_specs=[whole] * 2,
        out_shape=[
            jax.ShapeDtypeStruct((rows, width), jnp.float32),
            jax.ShapeDtypeStruct((rows, width), BF16),
        ],
        scratch_shapes=[
            pltpu.VMEM((parts, slots, width // parts), BF16),
            pltpu.SemaphoreType.DMA((parts,)),
        ],
        compiler_params=pltpu.CompilerParams(vmem_limit_bytes=16 * 2**20),
        cost_estimate=pl.CostEstimate(
            flops=8 * rows * slots * width, bytes_accessed=8 * 2**20, transcendentals=0
        ),
        name="combined",
    )(weights, returned)


def slots_of_block(chosen_pair, gates_pair, first_row, row_count, most):
    local_row = chosen_pair - first_row
    is_mine = (local_row >= 0) & (local_row < row_count)
    capacity_ids = jnp.arange(chosen_pair.shape[1], dtype=jnp.int32)
    earlier = (capacity_ids[:, None] < capacity_ids[None, :]).astype(BF16)
    rank = jnp.dot(is_mine.astype(BF16), earlier, preferred_element_type=jnp.float32)
    matches = is_mine[:, None, :] & (
        rank.astype(jnp.int32)[:, None, :] == jnp.arange(most, dtype=jnp.int32)[None, :, None]
    )
    row = jnp.sum(jnp.where(matches, local_row[:, None, :] + 1, 0), axis=2) - 1
    gate = jnp.sum(jnp.where(matches, gates_pair[:, None, :], 0.0), axis=2)
    return row, gate


def on_device(
    head_outputs, out_weight, residual, norm_gain, chosen, gates, place, w_gate, w_up, w_down
):
    x_count = lax.axis_size("x")
    core_count = lax.axis_size("core")
    tensor_count = lax.axis_size("z") * lax.axis_size("y")
    x_at = lax.axis_index("x")
    core_at = lax.axis_index("core")
    owners = x_count * core_count * tensor_count
    row_count, _ = residual.shape
    experts = place.shape[0]
    capacity = chosen.shape[1]
    most = 2 * capacity // owners
    swap = [(i, core_count - 1 - i) for i in range(core_count)]

    projected = project(head_outputs, out_weight, row_count)
    layer_state = residual.astype(jnp.float32) + projected
    scale = lax.rsqrt(jnp.mean(layer_state * layer_state, axis=1, keepdims=True) + 1.0)
    normed = (layer_state * scale * norm_gain[None, :]).astype(BF16)

    by_x = jnp.arange(x_count, dtype=jnp.int32) * core_count + core_at
    pairs = (by_x[:, None] * (tensor_count // 2) + jnp.arange(tensor_count // 2, dtype=jnp.int32)).reshape(-1)
    pair_map = (place[None, :] == pairs[:, None]).astype(jnp.float32)
    chosen_pair = jnp.dot(
        pair_map, chosen.astype(jnp.float32), precision=lax.Precision.HIGHEST
    ).astype(jnp.int32)
    gates_pair = jnp.dot(pair_map, gates, precision=lax.Precision.HIGHEST)
    tensor_at = lax.axis_index("z") * lax.axis_size("y") + lax.axis_index("y")
    my_first = ((x_at * core_count + core_at) * tensor_count + tensor_at) * row_count
    other_first = ((x_at * core_count + 1 - core_at) * tensor_count + tensor_at) * row_count
    my_row, my_gate = slots_of_block(chosen_pair, gates_pair, my_first, row_count, most)
    other_row, other_gate = slots_of_block(chosen_pair, gates_pair, other_first, row_count, most)
    other_row = jnp.where(other_row >= 0, other_row + row_count, -1)
    units = 2 * most
    slot_row = jnp.concatenate([my_row, other_row], axis=1)
    slot_gate = jnp.concatenate([my_gate, other_gate], axis=1)
    slot_row = jnp.broadcast_to(slot_row[:, None], (experts // 2, 2, units)).reshape(-1)
    slot_gate = jnp.broadcast_to(slot_gate[:, None], (experts // 2, 2, units)).reshape(-1)
    row_ids = jnp.arange(2 * row_count, dtype=jnp.int32)
    selector = (slot_row[:, None] == row_ids[None, :]).astype(BF16)
    combine = jnp.where(slot_row[None, :] == row_ids[:, None], slot_gate[None, :], 0.0)
    combine_high = combine.astype(BF16)
    combine_low = (combine - combine_high.astype(jnp.float32)).astype(BF16)
    combine = jnp.concatenate([combine_high, combine_low], axis=0)

    both = jnp.concatenate([normed, lax.ppermute(normed, "core", swap)], axis=0)
    outgoing = jnp.dot(selector, both, preferred_element_type=jnp.float32).astype(BF16)
    received = lax.all_to_all(outgoing, ROUTE, split_axis=0, concat_axis=0, tiled=True)

    contract = (((1,), (1,)), ((), ()))
    gate_part = lax.dot_general(received, w_gate[0], contract, preferred_element_type=jnp.float32)
    up_part = lax.dot_general(received, w_up[0], contract, preferred_element_type=jnp.float32)
    hidden = lax.optimization_barrier((jax.nn.silu(gate_part) * up_part).astype(BF16))
    result = jnp.dot(hidden, w_down[0], preferred_element_type=jnp.float32).astype(BF16)

    returned = lax.all_to_all(result, ROUTE, split_axis=0, concat_axis=0, tiled=True)
    moe, for_other = combined(combine, returned, row_count)
    from_other = lax.ppermute(for_other, "core", swap)
    return (layer_state + (moe + from_other.astype(jnp.float32))).astype(BF16)


def solution(mesh):
    dp, tensor = mesh.devices.shape
    side = round(tensor**0.5)
    split = jax.sharding.Mesh(mesh.devices.reshape(dp // 2, 2, side, side), ("x", "core", "z", "y"))
    rows = P(("x", "core", "z", "y"), None)
    weight = P(("x", "core", "z", "y"), None, None)
    return jax.shard_map(
        on_device,
        mesh=split,
        in_specs=(
            P(("x", "core"), ("z", "y")),
            P(("z", "y"), None),
            rows,
            P(),
            P(),
            P(),
            P(),
            weight,
            weight,
            weight,
        ),
        out_specs=rows,
        check_vma=False,
    )
```
